32 devices in a mesh: aa: 4 (over z), ba: 8 (over y, x, core).
Axes of the slice: x: 2, y: 2, z: 4, core: 2. Of those that a mesh axis runs over, the one named last changes fastest.
Arguments:
- deltas: bfloat16 [16384, 128], P(('aa', 'ba')), may hold values from -6 to 6
- row_ids: int32 [16384], P(('aa', 'ba')), may hold values from 0 to 4095, as said below
- sample_counts: int32 [16384], P(('aa', 'ba')), may hold values from 1 to 8
- live: int32 [16384], P(('aa', 'ba')), may hold values from 0 to 1, as said below
- table: float32 [131072, 128], P(('aa', 'ba')), may hold values from -6 to 6
- accum: float32 [131072, 128], P(('aa', 'ba')), may hold values from 0.01 to 1
Outputs:
- new_table: float32 [131072, 128], P(('aa', 'ba'))
- new_accum: float32 [131072, 128], P(('aa', 'ba'))
- fresh_rows: bfloat16 [16384, 128], P(('aa', 'ba'))
The draws below stay inside these ranges and needn't reach their ends.
Inputs may be any that keep to these rules, and one draw needn't show every extreme that they name: `row_ids`: A replica's 512 slots are 32 blocks of 16; block j holds rows of owner j, given as offsets among its 4096 rows, pairwise distinct within the block. In each block of 16 slots the live ones come first; every replica has some block with all 16 slots live.
All inputs are finite; a program needn't handle non-finite values.
Results may differ from the reference program's by a relative error of at most 0.0012.
Values may be sent and summed in bfloat16 or wider, within the bound.
No kernel may reach another device: no remote copies, remote signals or barrier semaphores. Data moves between devices by JAX's collectives and lax.ppermute only.
A program may use at most 64 MiB of HBM per device.

```python
import math
import jax
import jax.numpy as jnp

WIDTH = 128
ROWS_DEV = 4096
CAP = 16
REPLICAS = 32
SLOTS = 512
ROWS = 131072


def slot_layout(key):
    keys = jax.random.split(jax.random.fold_in(key, 71), 5)
    heat = jax.random.randint(keys[0], (REPLICAS,), 1, 5)
    spread = jax.random.randint(keys[1], (REPLICAS, REPLICAS), 0, max(1, CAP // 4) + 1)
    filled = CAP - spread * heat[None, :] // 4
    chosen = jax.random.randint(keys[2], (REPLICAS,), 0, REPLICAS)
    owners = jnp.arange(REPLICAS, dtype=jnp.int32)
    filled = jnp.where(owners[None, :] == chosen[:, None], CAP, filled)
    within = jnp.arange(CAP, dtype=jnp.int32)
    marks = (within[None, None, :] < filled[:, :, None]).astype(jnp.int32)
    anchor = jax.random.randint(keys[3], (REPLICAS, REPLICAS, 1), 0, ROWS_DEV)
    stride = jax.random.randint(keys[4], (REPLICAS, REPLICAS, 1), 0, ROWS_DEV // 2) * 2 + 1
    offset = (anchor + within[None, None, :] * stride) % ROWS_DEV
    return (offset.reshape(-1).astype(jnp.int32), marks.reshape(-1))


def draw_row_ids(key, part):
    return slot_layout(key)[0]


def draw_live(key, part):
    return slot_layout(key)[1]


def place_ends(array, own_key, least, largest):
    index_at = [jax.random.randint(jax.random.fold_in(own_key, axis), (), 0, length) for axis, length in enumerate(array.shape)]
    widest = array.shape.index(max(array.shape))
    next_to = index_at[:widest] + [(index_at[widest] + 1) % array.shape[widest]] + index_at[widest + 1:]
    return array.at[tuple(index_at)].set(least).at[tuple(next_to)].set(largest)


def steps_of(own_key, extent, cuts, least, top_value):
    loudness, own = 1.0, jax.random.fold_in(own_key, 6)
    for dim, parts in cuts:
        heights = jnp.exp(jax.random.uniform(jax.random.fold_in(own, dim), (parts,), jnp.float32, least / len(cuts), top_value / len(cuts)))
        loudness = loudness * jnp.repeat(heights, extent[dim] // parts).reshape([-1 if axis == dim else 1 for axis in range(len(extent))])
    return loudness


def scatter_about(stream_key, extent, scale, reach, cuts=(), held_as=jnp.bfloat16):
    entries = scale * jax.random.normal(stream_key, extent, jnp.float32)
    if cuts:
        entries = entries * steps_of(stream_key, extent, cuts, -0.22, 0.18)
    return jnp.clip(entries, -reach, reach).astype(held_as)


def setup_inputs(seed: int = 0) -> dict:
    splits = jax.random.split(jax.random.key(seed), 7)
    return {
        "deltas": scatter_about(splits[0], (REPLICAS * SLOTS, WIDTH), 1.0, 6.0, ((0, 32),)),
        "row_ids": draw_row_ids(jax.random.fold_in(splits[6], 71), 0),
        "sample_counts": place_ends(jax.random.randint(splits[2], (REPLICAS * SLOTS,), 1, 9), jax.random.fold_in(splits[2], 1), 1, 8).astype(jnp.int32),
        "live": draw_live(jax.random.fold_in(splits[6], 71), 0),
        "table": scatter_about(splits[4], (ROWS, WIDTH), 1.0, 6.0, ((0, 32),), jnp.float32),
        "accum": jnp.clip(jnp.exp(math.log(1.0) - 4.6051702 * jax.random.uniform(splits[5], (ROWS, WIDTH), jnp.float32) ** steps_of(splits[5], (ROWS, WIDTH), ((0, 32),), -0.2, 0.2)), 0.01, 1.0),
    }


learn_rate = 0.1
epsilon = 1e-08

def reference(deltas, row_ids, sample_counts, live, table, accum):
    count = row_ids.shape[0]
    position = jnp.arange(count, dtype=jnp.int32)
    row = (position // CAP % REPLICAS).astype(jnp.int32) * ROWS_DEV + row_ids.astype(jnp.int32)
    weight = (sample_counts * live).astype(jnp.float32)
    terms = deltas.astype(jnp.float32) * weight[:, None]
    numer = jax.ops.segment_sum(terms, row, num_segments=table.shape[0])
    total = jax.ops.segment_sum(weight, row, num_segments=table.shape[0])
    grad = numer / jnp.maximum(total, 1.0)[:, None]
    new_accum = accum + grad * grad
    new_table = table - learn_rate * grad / (jnp.sqrt(new_accum) + epsilon)
    fresh_rows = new_table[row].astype(jnp.bfloat16)
    return (new_table, new_accum, fresh_rows)
```

```python
import functools

import jax
import jax.numpy as jnp
from jax import lax
from jax.experimental import pallas as pl
from jax.experimental.pallas import tpu as pltpu
from jax.sharding import PartitionSpec as P

learn_rate = 0.1
epsilon = 1e-08

LANES = 128
TAG_ROWS = 8
DIGIT = 256
SLOT_BLOCK = 512
COPIES = 4


def pack_kernel(cap, deltas_ref, ids_ref, counts_ref, live_ref, out_ref):
    per = LANES // cap
    n_dest, _, width = out_ref.shape
    out_ref[:, 0:cap, :] = deltas_ref[...].reshape(n_dest, cap, width)
    sub = lax.broadcasted_iota(jnp.int32, (TAG_ROWS, LANES), 0)
    for r in range(n_dest // per):
        lanes = pl.ds(r * LANES, LANES)
        ids = ids_ref[lanes][None, :]
        weight = (counts_ref[lanes] * live_ref[lanes])[None, :]
        upper = lax.shift_right_logical(ids, 8)
        lower = jnp.bitwise_and(ids, DIGIT - 1)
        tag = jnp.where(sub == 0, upper, jnp.where(sub == 1, lower, jnp.where(sub == 2, weight, 0)))
        tag = tag.astype(jnp.float32).astype(jnp.bfloat16)
        out_ref[pl.ds(r * per, per), cap : cap + TAG_ROWS, :] = jnp.broadcast_to(
            tag[None], (per, TAG_ROWS, LANES)
        )


def copies(src, dst, sem):
    rows = src.shape[0] // COPIES
    return [
        pltpu.make_async_copy(
            src.at[pl.ds(i * rows, rows)], dst.at[pl.ds(i * rows, rows)], sem.at[i]
        )
        for i in range(COPIES)
    ]


def slots_kernel(
    cap, me_ref, got_ref, table_hbm, accum_hbm,
    reply_ref, new_t_ref, new_a_ref, ids_ref,
    tab, acc, id_row, id_smem, picked_t, picked_a, sem_t, sem_a, sem_i,
):
    loads = copies(table_hbm, tab, sem_t) + copies(accum_hbm, acc, sem_a)
    for load in loads:
        load.start()
    n_src, _, width = got_ref.shape
    n = n_src * cap
    per = LANES // cap
    first = lax.rem(me_ref[0], per) * cap
    lane = lax.broadcasted_iota(jnp.int32, (n_src, cap, LANES), 2)
    slot = lax.broadcasted_iota(jnp.int32, (n_src, cap, LANES), 1)
    mine = lane == slot + first
    tags = got_ref[:, cap : cap + TAG_ROWS, :].astype(jnp.float32)

    def spread(i):
        own = jnp.where(mine, tags[:, i : i + 1, :], 0.0)
        return own.reshape(n, LANES).astype(jnp.bfloat16)

    upper, lower, weight = spread(0), spread(1), spread(2)
    ones = jnp.ones((LANES, LANES), jnp.bfloat16)
    one_row = jnp.ones((8, LANES), jnp.bfloat16)
    f32 = jnp.float32

    def down(x):
        return jnp.dot(x, ones, preferred_element_type=f32)

    def across(x):
        return lax.dot_general(one_row, x, (((1,), (1,)), ((), ())), preferred_element_type=f32)

    row_f = across(upper) * DIGIT + across(lower)
    id_row[...] = row_f.astype(jnp.int32)
    ids_copy = pltpu.make_async_copy(id_row.at[pl.ds(0, 1)], id_smem, sem_i)
    ids_copy.start()
    column = down(upper) * DIGIT + down(lower)
    row_f, weight_row = row_f[0:1], across(weight)[0:1]
    deltas = got_ref[:, 0:cap, :].reshape(n, width)
    values = jnp.concatenate([deltas, jnp.ones((n, LANES), jnp.bfloat16)], axis=1)
    block = min(SLOT_BLOCK, n)
    sums = []
    for b in range(n // block):
        mark = jnp.concatenate([column[b * block : (b + 1) * block]] * (n // LANES), axis=1)
        weighted = jnp.where(mark == row_f, weight_row, 0.0).astype(jnp.bfloat16)
        sums.append(jnp.dot(weighted, values, preferred_element_type=f32))
    ids_copy.wait()
    for load in loads:
        load.wait()

    def pick(s, carry):
        v = id_smem[0, s]
        ids_ref[0, s] = v
        picked_t[pl.ds(s, 1), :] = tab[pl.ds(v, 1), :]
        picked_a[pl.ds(s, 1), :] = acc[pl.ds(v, 1), :]
        return carry

    lax.fori_loop(0, n, pick, 0, unroll=16)
    for b in range(n // block):
        part = pl.ds(b * block, block)
        grad = sums[b][:, 0:width] / jnp.maximum(sums[b][:, width : width + LANES], 1.0)
        next_a = picked_a[part] + grad * grad
        next_t = picked_t[part] - learn_rate * grad / (jnp.sqrt(next_a) + epsilon)
        new_a_ref[part] = next_a
        new_t_ref[part] = next_t
        reply_ref[part] = next_t.astype(jnp.bfloat16)


def write_kernel(
    ids_ref, new_t_ref, new_a_ref, table_hbm, accum_hbm, out_t, out_a,
    tab, acc, sem_t, sem_a,
):
    loads = copies(table_hbm, tab, sem_t) + copies(accum_hbm, acc, sem_a)
    for load in loads:
        load.start()
    for load in loads:
        load.wait()

    def put(s, carry):
        v = ids_ref[0, s]
        tab[pl.ds(v, 1), :] = new_t_ref[pl.ds(s, 1), :]
        acc[pl.ds(v, 1), :] = new_a_ref[pl.ds(s, 1), :]
        return carry

    lax.fori_loop(0, new_t_ref.shape[0], put, 0, unroll=16)
    stores = copies(tab, out_t, sem_t) + copies(acc, out_a, sem_a)
    for store in stores:
        store.start()
    for store in stores:
        store.wait()


def on_device(deltas, row_ids, sample_counts, live, table, accum):
    axes = ("aa", "ba")
    n_dest = lax.axis_size(axes)
    width = deltas.shape[1]
    n = deltas.shape[0]
    cap = n // n_dest
    vmem = pl.BlockSpec(memory_space=pltpu.VMEM)
    smem = pl.BlockSpec(memory_space=pltpu.SMEM)
    anywhere = pl.BlockSpec(memory_space=pl.ANY)
    f32 = jnp.float32
    payload = pl.pallas_call(
        functools.partial(pack_kernel, cap),
        out_shape=jax.ShapeDtypeStruct((n_dest, cap + TAG_ROWS, width), jnp.bfloat16),
        in_specs=[vmem] * 4,
        out_specs=vmem,
        name="pack",
    )(deltas, row_ids, sample_counts, live)
    got = lax.all_to_all(payload, axes, split_axis=0, concat_axis=0, tiled=True)
    me = lax.axis_index(axes).astype(jnp.int32).reshape(1)
    rows = jax.ShapeDtypeStruct((n, width), f32)
    held = [pltpu.VMEM(table.shape, f32), pltpu.VMEM(accum.shape, f32)]
    replies, new_t, new_a, ids = pl.pallas_call(
        functools.partial(slots_kernel, cap),
        out_shape=(
            jax.ShapeDtypeStruct((n, width), jnp.bfloat16), rows, rows,
            jax.ShapeDtypeStruct((1, n), jnp.int32),
        ),
        in_specs=[smem, vmem, anywhere, anywhere],
        out_specs=(vmem, vmem, vmem, smem),
        scratch_shapes=held + [
            pltpu.VMEM((8, n), jnp.int32), pltpu.SMEM((1, n), jnp.int32),
            pltpu.VMEM((n, width), f32), pltpu.VMEM((n, width), f32),
            pltpu.SemaphoreType.DMA((COPIES,)), pltpu.SemaphoreType.DMA((COPIES,)),
            pltpu.SemaphoreType.DMA,
        ],
        name="slots",
    )(me, got, table, accum)
    returned = lax.all_to_all(
        replies.reshape(n_dest, cap, width), axes, split_axis=0, concat_axis=0, tiled=True
    )
    new_table, new_accum = pl.pallas_call(
        write_kernel,
        out_shape=(
            jax.ShapeDtypeStruct(table.shape, f32), jax.ShapeDtypeStruct(accum.shape, f32),
        ),
        in_specs=[smem, vmem, vmem, anywhere, anywhere],
        out_specs=(anywhere, anywhere),
        scratch_shapes=held + [
            pltpu.SemaphoreType.DMA((COPIES,)), pltpu.SemaphoreType.DMA((COPIES,)),
        ],
        cost_estimate=pl.CostEstimate(flops=10**9, transcendentals=0, bytes_accessed=8 * 2**20),
        name="write",
    )(ids, new_t, new_a, table, accum)
    return (new_table, new_accum, returned.reshape(-1, width))


def solution(mesh):
    placed = (
        P(("aa", "ba"), None),
        P(("aa", "ba")),
        P(("aa", "ba")),
        P(("aa", "ba")),
        P(("aa", "ba"), None),
        P(("aa", "ba"), None),
    )
    return jax.shard_map(
        on_device,
        mesh=mesh,
        in_specs=placed,
        out_specs=(P(("aa", "ba"), None), P(("aa", "ba"), None), P(("aa", "ba"), None)),
        check_vma=False,
    )
```

```python
import functools

import jax
import jax.numpy as jnp
from jax import lax
from jax.experimental import pallas as pl
from jax.experimental.pallas import tpu as pltpu
from jax.sharding import PartitionSpec as P

learn_rate = 0.1
epsilon = 1e-08

LANES = 128
TAG_ROWS = 8
DIGIT = 256
SLOT_BLOCK = 512
COPIES = 4
MIB = 2**20
PACK_VMEM = 8 * MIB


def pack_kernel(
    cap, deltas_hbm, ids_hbm, counts_hbm, live_hbm, out_ref, ids_ref, counts_ref, live_ref, sem
):
    per = LANES // cap
    n_dest = out_ref.shape[0]
    loads = [
        pltpu.make_async_copy(ids_hbm, ids_ref, sem.at[0]),
        pltpu.make_async_copy(counts_hbm, counts_ref, sem.at[1]),
        pltpu.make_async_copy(live_hbm, live_ref, sem.at[2]),
        pltpu.make_async_copy(deltas_hbm, out_ref.at[:, pl.ds(0, cap), :], sem.at[3]),
    ]
    for load in loads:
        load.start()
    for load in loads[:3]:
        load.wait()
    sub = lax.broadcasted_iota(jnp.int32, (TAG_ROWS, LANES), 0)
    for r in range(n_dest // per):
        lanes = pl.ds(r * LANES, LANES)
        ids = ids_ref[lanes][None, :]
        weight = (counts_ref[lanes] * live_ref[lanes])[None, :]
        upper = lax.shift_right_logical(ids, 8)
        lower = jnp.bitwise_and(ids, DIGIT - 1)
        tag = jnp.where(sub == 0, upper, jnp.where(sub == 1, lower, jnp.where(sub == 2, weight, 0)))
        tag = tag.astype(jnp.float32).astype(jnp.bfloat16)
        out_ref[pl.ds(r * per, per), cap : cap + TAG_ROWS, :] = jnp.broadcast_to(
            tag[None], (per, TAG_ROWS, LANES)
        )
    loads[3].wait()


def copies(src, dst, sem):
    rows = src.shape[0] // COPIES
    return [
        pltpu.make_async_copy(
            src.at[pl.ds(i * rows, rows)], dst.at[pl.ds(i * rows, rows)], sem.at[i]
        )
        for i in range(COPIES)
    ]


def slots_kernel(
    cap, axes, got_ref, table_hbm, accum_hbm,
    reply_ref, new_t_ref, new_a_ref, ids_ref,
    tab, acc, id_row, id_smem, picked_t, picked_a, sem_t, sem_a, sem_i,
):
    loads = copies(table_hbm, tab, sem_t) + copies(accum_hbm, acc, sem_a)
    for load in loads:
        load.start()
    n_src, _, width = got_ref.shape
    n = n_src * cap
    per = LANES // cap
    first = lax.rem(lax.axis_index(axes), per) * cap
    lane = lax.broadcasted_iota(jnp.int32, (n_src, cap, LANES), 2)
    slot = lax.broadcasted_iota(jnp.int32, (n_src, cap, LANES), 1)
    mine = lane == slot + first
    tags = got_ref[:, cap : cap + TAG_ROWS, :].astype(jnp.float32)

    def spread(i):
        own = jnp.where(mine, tags[:, i : i + 1, :], 0.0)
        return own.reshape(n, LANES).astype(jnp.bfloat16)

    upper, lower, weight = spread(0), spread(1), spread(2)
    ones = jnp.ones((LANES, LANES), jnp.bfloat16)
    one_row = jnp.ones((8, LANES), jnp.bfloat16)
    f32 = jnp.float32

    def down(x):
        return jnp.dot(x, ones, preferred_element_type=f32)

    def across(x):
        return lax.dot_general(one_row, x, (((1,), (1,)), ((), ())), preferred_element_type=f32)

    row_f = across(upper) * DIGIT + across(lower)
    id_row[...] = row_f.astype(jnp.int32)
    ids_copy = pltpu.make_async_copy(id_row.at[pl.ds(0, 1)], id_smem, sem_i)
    ids_copy.start()
    column = down(upper) * DIGIT + down(lower)
    row_f, weight_row = row_f[0:1], across(weight)[0:1]
    deltas = got_ref[:, 0:cap, :].reshape(n, width)
    values = jnp.concatenate([deltas, jnp.ones((n, LANES), jnp.bfloat16)], axis=1)
    block = min(SLOT_BLOCK, n)
    sums = []
    for b in range(n // block):
        mark = jnp.concatenate([column[b * block : (b + 1) * block]] * (n // LANES), axis=1)
        weighted = jnp.where(mark == row_f, weight_row, 0.0).astype(jnp.bfloat16)
        sums.append(jnp.dot(weighted, values, preferred_element_type=f32))
    ids_copy.wait()
    for load in loads:
        load.wait()

    def pick(s, carry):
        v = id_smem[0, s]
        ids_ref[0, s] = v
        picked_t[pl.ds(s, 1), :] = tab[pl.ds(v, 1), :]
        picked_a[pl.ds(s, 1), :] = acc[pl.ds(v, 1), :]
        return carry

    lax.fori_loop(0, n, pick, 0, unroll=16)
    for b in range(n // block):
        part = pl.ds(b * block, block)
        grad = sums[b][:, 0:width] / jnp.maximum(sums[b][:, width : width + LANES], 1.0)
        next_a = picked_a[part] + grad * grad
        next_t = picked_t[part] - learn_rate * grad / (jnp.sqrt(next_a) + epsilon)
        new_a_ref[part] = next_a
        new_t_ref[part] = next_t
        reply_ref[part] = next_t.astype(jnp.bfloat16)


def write_kernel(
    ids_ref, new_t_ref, new_a_ref, table_hbm, accum_hbm, out_t, out_a,
    tab, acc, sem_t, sem_a,
):
    loads = copies(table_hbm, tab, sem_t) + copies(accum_hbm, acc, sem_a)
    for load in loads:
        load.start()
    for load in loads:
        load.wait()

    def put(s, carry):
        v = ids_ref[0, s]
        tab[pl.ds(v, 1), :] = new_t_ref[pl.ds(s, 1), :]
        acc[pl.ds(v, 1), :] = new_a_ref[pl.ds(s, 1), :]
        return carry

    lax.fori_loop(0, new_t_ref.shape[0], put, 0, unroll=16)
    stores = copies(tab, out_t, sem_t) + copies(acc, out_a, sem_a)
    for store in stores:
        store.start()
    for store in stores:
        store.wait()


def in_hbm(*arrays):
    return [pltpu.with_memory_space_constraint(x, pltpu.HBM) for x in arrays]


def on_device(deltas, row_ids, sample_counts, live, table, accum):
    axes = ("aa", "ba")
    n_dest = lax.axis_size(axes)
    width = deltas.shape[1]
    n = deltas.shape[0]
    cap = n // n_dest
    vmem = pl.BlockSpec(memory_space=pltpu.VMEM)
    smem = pl.BlockSpec(memory_space=pltpu.SMEM)
    hbm = pl.BlockSpec(memory_space=pltpu.HBM)
    f32 = jnp.float32
    slots_vmem = 16 * MIB if n <= SLOT_BLOCK else 60 * MIB
    write_vmem = 16 * MIB
    payload = pl.pallas_call(
        functools.partial(pack_kernel, cap),
        out_shape=jax.ShapeDtypeStruct((n_dest, cap + TAG_ROWS, width), jnp.bfloat16),
        in_specs=[hbm] * 4,
        out_specs=vmem,
        scratch_shapes=[pltpu.VMEM((n,), jnp.int32)] * 3 + [pltpu.SemaphoreType.DMA((4,))],
        compiler_params=pltpu.CompilerParams(vmem_limit_bytes=PACK_VMEM),
        name="pack",
    )(*in_hbm(deltas.reshape(n_dest, cap, width), row_ids, sample_counts, live))
    got = lax.all_to_all(payload, axes, split_axis=0, concat_axis=0, tiled=True)
    rows = jax.ShapeDtypeStruct((n, width), f32)
    held = [pltpu.VMEM(table.shape, f32), pltpu.VMEM(accum.shape, f32)]
    replies, new_t, new_a, ids = pl.pallas_call(
        functools.partial(slots_kernel, cap, axes),
        out_shape=(
            jax.ShapeDtypeStruct((n, width), jnp.bfloat16), rows, rows,
            jax.ShapeDtypeStruct((1, n), jnp.int32),
        ),
        in_specs=[vmem, hbm, hbm],
        out_specs=(vmem, vmem, vmem, smem),
        scratch_shapes=held + [
            pltpu.VMEM((8, n), jnp.int32), pltpu.SMEM((1, n), jnp.int32),
            pltpu.VMEM((n, width), f32), pltpu.VMEM((n, width), f32),
            pltpu.SemaphoreType.DMA((COPIES,)), pltpu.SemaphoreType.DMA((COPIES,)),
            pltpu.SemaphoreType.DMA,
        ],
        compiler_params=pltpu.CompilerParams(vmem_limit_bytes=slots_vmem),
        name="slots",
    )(got, *in_hbm(table, accum))
    returned = lax.all_to_all(
        replies.reshape(n_dest, cap, width), axes, split_axis=0, concat_axis=0, tiled=True
    )
    new_table, new_accum = pl.pallas_call(
        write_kernel,
        out_shape=(
            jax.ShapeDtypeStruct(table.shape, f32), jax.ShapeDtypeStruct(accum.shape, f32),
        ),
        in_specs=[smem, vmem, vmem, hbm, hbm],
        out_specs=(hbm, hbm),
        scratch_shapes=held + [
            pltpu.SemaphoreType.DMA((COPIES,)), pltpu.SemaphoreType.DMA((COPIES,)),
        ],
        cost_estimate=pl.CostEstimate(flops=10**9, transcendentals=0, bytes_accessed=8 * 2**20),
        compiler_params=pltpu.CompilerParams(vmem_limit_bytes=write_vmem),
        name="write",
    )(ids, new_t, new_a, *in_hbm(table, accum))
    return (new_table, new_accum, returned.reshape(-1, width))


def solution(mesh):
    placed = (
        P(("aa", "ba"), None),
        P(("aa", "ba")),
        P(("aa", "ba")),
        P(("aa", "ba")),
        P(("aa", "ba"), None),
        P(("aa", "ba"), None),
    )
    return jax.shard_map(
        on_device,
        mesh=mesh,
        in_specs=placed,
        out_specs=(P(("aa", "ba"), None), P(("aa", "ba"), None), P(("aa", "ba"), None)),
        check_vma=False,
    )
```

```python
import functools

import jax
import jax.numpy as jnp
from jax import lax
from jax.experimental import pallas as pl
from jax.experimental.pallas import tpu as pltpu
from jax.sharding import PartitionSpec as P

learn_rate = 0.1
epsilon = 1e-08

LANES = 128
TAG_ROWS = 8
DIGIT = 256
SLOT_BLOCK = 512
COPIES = 4
MIB = 2**20
PACK_VMEM = 8 * MIB


def pack_kernel(
    cap, deltas_hbm, ids_hbm, counts_hbm, live_hbm, out_ref, ids_ref, counts_ref, live_ref, sem
):
    per = LANES // cap
    n_dest = out_ref.shape[0]
    loads = [
        pltpu.make_async_copy(ids_hbm, ids_ref, sem.at[0]),
        pltpu.make_async_copy(counts_hbm, counts_ref, sem.at[1]),
        pltpu.make_async_copy(live_hbm, live_ref, sem.at[2]),
        pltpu.make_async_copy(deltas_hbm, out_ref.at[:, pl.ds(0, cap), :], sem.at[3]),
    ]
    for load in loads:
        load.start()
    for load in loads[:3]:
        load.wait()
    sub = lax.broadcasted_iota(jnp.int32, (TAG_ROWS, LANES), 0)
    for r in range(n_dest // per):
        lanes = pl.ds(r * LANES, LANES)
        ids = ids_ref[lanes][None, :]
        weight = (counts_ref[lanes] * live_ref[lanes])[None, :]
        upper = lax.shift_right_logical(ids, 8)
        lower = jnp.bitwise_and(ids, DIGIT - 1)
        tag = jnp.where(sub == 0, upper, jnp.where(sub == 1, lower, jnp.where(sub == 2, weight, 0)))
        tag = tag.astype(jnp.float32).astype(jnp.bfloat16)
        out_ref[pl.ds(r * per, per), cap : cap + TAG_ROWS, :] = jnp.broadcast_to(
            tag[None], (per, TAG_ROWS, LANES)
        )
    loads[3].wait()


def copies(src, dst, sem):
    rows = src.shape[0] // COPIES
    return [
        pltpu.make_async_copy(
            src.at[pl.ds(i * rows, rows)], dst.at[pl.ds(i * rows, rows)], sem.at[i]
        )
        for i in range(COPIES)
    ]


def slots_kernel(
    cap, axes, got_ref, table_ref, accum_ref, reply_ref, new_t_ref, new_a_ref, ids_ref,
    id_smem, picked_t, picked_a, sem_i,
):
    n_src, _, width = got_ref.shape
    n = n_src * cap
    per = LANES // cap
    first = lax.rem(lax.axis_index(axes), per) * cap
    lane = lax.broadcasted_iota(jnp.int32, (n_src, cap, LANES), 2)
    slot = lax.broadcasted_iota(jnp.int32, (n_src, cap, LANES), 1)
    mine = lane == slot + first
    tags = got_ref[:, cap : cap + TAG_ROWS, :].astype(jnp.float32)

    def spread(i):
        own = jnp.where(mine, tags[:, i : i + 1, :], 0.0)
        return own.reshape(n, LANES).astype(jnp.bfloat16)

    upper, lower, weight = spread(0), spread(1), spread(2)
    ones = jnp.ones((LANES, LANES), jnp.bfloat16)
    one_row = jnp.ones((8, LANES), jnp.bfloat16)
    f32 = jnp.float32

    def down(x):
        return jnp.dot(x, ones, preferred_element_type=f32)

    def across(x):
        return lax.dot_general(one_row, x, (((1,), (1,)), ((), ())), preferred_element_type=f32)

    row_f = across(upper) * DIGIT + across(lower)
    ids_ref[...] = row_f.astype(jnp.int32)
    ids_copy = pltpu.make_async_copy(ids_ref.at[pl.ds(0, 1)], id_smem, sem_i)
    ids_copy.start()
    column = down(upper) * DIGIT + down(lower)
    row_f, weight_row = row_f[0:1], across(weight)[0:1]
    deltas = got_ref[:, 0:cap, :].reshape(n, width)
    values = jnp.concatenate([deltas, jnp.ones((n, LANES), jnp.bfloat16)], axis=1)
    block = min(SLOT_BLOCK, n)
    sums = []
    for b in range(n // block):
        mark = jnp.concatenate([column[b * block : (b + 1) * block]] * (n // LANES), axis=1)
        weighted = jnp.where(mark == row_f, weight_row, 0.0).astype(jnp.bfloat16)
        sums.append(jnp.dot(weighted, values, preferred_element_type=f32))
    ids_copy.wait()

    def pick_t(s, carry):
        picked_t[pl.ds(s, 1), :] = table_ref[pl.ds(id_smem[0, s], 1), :]
        return carry

    def pick_a(s, carry):
        picked_a[pl.ds(s, 1), :] = accum_ref[pl.ds(id_smem[0, s], 1), :]
        return carry

    lax.fori_loop(0, n, pick_t, 0, unroll=32)
    lax.fori_loop(0, n, pick_a, 0, unroll=32)
    for b in range(n // block):
        part = pl.ds(b * block, block)
        grad = sums[b][:, 0:width] / jnp.maximum(sums[b][:, width : width + LANES], 1.0)
        next_a = picked_a[part] + grad * grad
        next_t = picked_t[part] - learn_rate * grad / (jnp.sqrt(next_a) + epsilon)
        new_a_ref[part] = next_a
        new_t_ref[part] = next_t
        reply_ref[part] = next_t.astype(jnp.bfloat16)


def write_kernel(
    ids_ref, new_t_ref, new_a_ref, table_hbm, accum_hbm, out_t, out_a,
    id_smem, tab, acc, sem_t, sem_a, sem_i,
):
    loads = copies(table_hbm, tab, sem_t) + copies(accum_hbm, acc, sem_a)
    for load in loads:
        load.start()
    ids_copy = pltpu.make_async_copy(ids_ref.at[pl.ds(0, 1)], id_smem, sem_i)
    ids_copy.start()
    ids_copy.wait()
    for load in loads:
        load.wait()

    def put_t(s, carry):
        tab[pl.ds(id_smem[0, s], 1), :] = new_t_ref[pl.ds(s, 1), :]
        return carry

    def put_a(s, carry):
        acc[pl.ds(id_smem[0, s], 1), :] = new_a_ref[pl.ds(s, 1), :]
        return carry

    lax.fori_loop(0, new_t_ref.shape[0], put_t, 0, unroll=32)
    lax.fori_loop(0, new_t_ref.shape[0], put_a, 0, unroll=32)
    stores = copies(tab, out_t, sem_t) + copies(acc, out_a, sem_a)
    for store in stores:
        store.start()
    for store in stores:
        store.wait()


def in_hbm(*arrays):
    return [pltpu.with_memory_space_constraint(x, pltpu.HBM) for x in arrays]


def on_device(deltas, row_ids, sample_counts, live, table, accum):
    axes = ("aa", "ba")
    n_dest = lax.axis_size(axes)
    width = deltas.shape[1]
    n = deltas.shape[0]
    cap = n // n_dest
    vmem = pl.BlockSpec(memory_space=pltpu.VMEM)
    hbm = pl.BlockSpec(memory_space=pltpu.HBM)
    f32 = jnp.float32
    slots_vmem = 16 * MIB if n <= SLOT_BLOCK else 60 * MIB
    write_vmem = 16 * MIB
    payload = pl.pallas_call(
        functools.partial(pack_kernel, cap),
        out_shape=jax.ShapeDtypeStruct((n_dest, cap + TAG_ROWS, width), jnp.bfloat16),
        in_specs=[hbm] * 4,
        out_specs=vmem,
        scratch_shapes=[pltpu.VMEM((n,), jnp.int32)] * 3 + [pltpu.SemaphoreType.DMA((4,))],
        compiler_params=pltpu.CompilerParams(vmem_limit_bytes=PACK_VMEM),
        cost_estimate=pl.CostEstimate(flops=10**10, transcendentals=0, bytes_accessed=2**24),
        name="pack",
    )(*in_hbm(deltas.reshape(n_dest, cap, width), row_ids, sample_counts, live))
    got = lax.all_to_all(payload, axes, split_axis=0, concat_axis=0, tiled=True)
    rows = jax.ShapeDtypeStruct((n, width), f32)
    held = [pltpu.VMEM(table.shape, f32), pltpu.VMEM(accum.shape, f32)]
    replies, new_t, new_a, ids = pl.pallas_call(
        functools.partial(slots_kernel, cap, axes),
        out_shape=(
            jax.ShapeDtypeStruct((n, width), jnp.bfloat16), rows, rows,
            jax.ShapeDtypeStruct((8, n), jnp.int32),
        ),
        in_specs=[vmem] * 3,
        out_specs=(vmem,) * 4,
        scratch_shapes=[
            pltpu.SMEM((1, n), jnp.int32), pltpu.VMEM((n, width), f32),
            pltpu.VMEM((n, width), f32), pltpu.SemaphoreType.DMA,
        ],
        compiler_params=pltpu.CompilerParams(vmem_limit_bytes=slots_vmem),
        name="slots",
    )(got, table, accum)
    returned = lax.all_to_all(
        replies.reshape(n_dest, cap, width), axes, split_axis=0, concat_axis=0, tiled=True
    )
    new_table, new_accum = pl.pallas_call(
        write_kernel,
        out_shape=(
            jax.ShapeDtypeStruct(table.shape, f32), jax.ShapeDtypeStruct(accum.shape, f32),
        ),
        in_specs=[vmem, vmem, vmem, hbm, hbm],
        out_specs=(hbm, hbm),
        scratch_shapes=[pltpu.SMEM((1, n), jnp.int32)] + held + [
            pltpu.SemaphoreType.DMA((COPIES,)), pltpu.SemaphoreType.DMA((COPIES,)),
            pltpu.SemaphoreType.DMA,
        ],
        cost_estimate=pl.CostEstimate(flops=10**9, transcendentals=0, bytes_accessed=8 * 2**20),
        compiler_params=pltpu.CompilerParams(vmem_limit_bytes=write_vmem),
        name="write",
    )(ids, new_t, new_a, *in_hbm(table, accum))
    return (new_table, new_accum, returned.reshape(-1, width))


def solution(mesh):
    placed = (
        P(("aa", "ba"), None),
        P(("aa", "ba")),
        P(("aa", "ba")),
        P(("aa", "ba")),
        P(("aa", "ba"), None),
        P(("aa", "ba"), None),
    )
    return jax.shard_map(
        on_device,
        mesh=mesh,
        in_specs=placed,
        out_specs=(P(("aa", "ba"), None), P(("aa", "ba"), None), P(("aa", "ba"), None)),
        check_vma=False,
    )
```

```python
import functools

import jax
import jax.numpy as jnp
from jax import lax
from jax.experimental import pallas as pl
from jax.experimental.pallas import tpu as pltpu
from jax.sharding import PartitionSpec as P

learn_rate = 0.1
epsilon = 1e-08

LANES = 128
SUBLANES = 8
GROUP = 16
TAG_ROWS = 8
DIGIT = 256
SLOT_BLOCK = 512
COPIES = 4
MIB = 2**20
PACK_VMEM = 8 * MIB


def pack_kernel(
    cap, deltas_hbm, ids_hbm, counts_hbm, live_hbm, out_ref, ids_ref, counts_ref, live_ref, sem
):
    per = LANES // cap
    n_dest = out_ref.shape[0]
    loads = [
        pltpu.make_async_copy(ids_hbm, ids_ref, sem.at[0]),
        pltpu.make_async_copy(counts_hbm, counts_ref, sem.at[1]),
        pltpu.make_async_copy(live_hbm, live_ref, sem.at[2]),
        pltpu.make_async_copy(deltas_hbm, out_ref.at[:, pl.ds(0, cap), :], sem.at[3]),
    ]
    for load in loads:
        load.start()
    for load in loads[:3]:
        load.wait()
    sub = lax.broadcasted_iota(jnp.int32, (TAG_ROWS, LANES), 0)
    for r in range(n_dest // per):
        lanes = pl.ds(r * LANES, LANES)
        ids = ids_ref[lanes][None, :]
        weight = (counts_ref[lanes] * live_ref[lanes])[None, :]
        upper = lax.shift_right_logical(ids, 8)
        lower = jnp.bitwise_and(ids, DIGIT - 1)
        tag = jnp.where(sub == 0, upper, jnp.where(sub == 1, lower, jnp.where(sub == 2, weight, 0)))
        tag = tag.astype(jnp.float32).astype(jnp.bfloat16)
        out_ref[pl.ds(r * per, per), cap : cap + TAG_ROWS, :] = jnp.broadcast_to(
            tag[None], (per, TAG_ROWS, LANES)
        )
    loads[3].wait()


def copies(src, dst, sem):
    rows = src.shape[0] // COPIES
    return [
        pltpu.make_async_copy(
            src.at[pl.ds(i * rows, rows)], dst.at[pl.ds(i * rows, rows)], sem.at[i]
        )
        for i in range(COPIES)
    ]


def gather_ids(cap, axes, got_ref, id_rows, id_smem, sem):
    n_src = got_ref.shape[0]
    per = LANES // cap
    mine = lax.rem(lax.axis_index(axes), per)
    lane = lax.broadcasted_iota(jnp.int32, (TAG_ROWS, LANES), 1)
    own = lane // cap == mine
    ids, weights = [], []
    for r in range(n_src // per):
        tile = jnp.zeros((TAG_ROWS, LANES), jnp.float32)
        for k in range(per):
            tag = got_ref[r * per + k, cap : cap + TAG_ROWS, :].astype(jnp.float32)
            shift = lax.rem(k - mine + per, per) * cap
            tile = tile + pltpu.roll(jnp.where(own, tag, 0.0), shift, 1)
        row = tile[0:1] * DIGIT + tile[1:2]
        id_rows[r : r + 1] = row.astype(jnp.int32)
        ids.append(row)
        weights.append(tile[2:3])
    copy = pltpu.make_async_copy(id_rows, id_smem, sem)
    copy.start()
    return jnp.concatenate(ids, axis=1), jnp.concatenate(weights, axis=1), copy


def each_slot(n, body):
    block = min(SLOT_BLOCK, n)

    def one_block(b):
        for k in range(block):
            s = b * block + k
            body(s, s // LANES, s % LANES)

    if n == block:
        one_block(0)
    else:

        def step(s, carry):
            body(s, s // LANES, lax.rem(s, LANES))
            return carry

        lax.fori_loop(0, n, step, 0, unroll=32)


def slots_kernel(
    cap, axes, got_ref, table_ref, accum_ref, reply_ref, new_t_ref, new_a_ref, ids_ref,
    id_smem, sums, sem_i,
):
    n_src, _, width = got_ref.shape
    n = n_src * cap
    row_f, weight_row, ids_copy = gather_ids(cap, axes, got_ref, ids_ref, id_smem, sem_i)
    per = LANES // cap
    first = lax.rem(lax.axis_index(axes), per) * cap
    lane = lax.broadcasted_iota(jnp.int32, (n_src, cap, LANES), 2)
    slot = lax.broadcasted_iota(jnp.int32, (n_src, cap, LANES), 1)
    mine = lane == slot + first
    tags = got_ref[:, cap : cap + TAG_ROWS, :].astype(jnp.float32)
    ones = jnp.ones((LANES, LANES), jnp.bfloat16)
    f32 = jnp.float32

    def down(i):
        own = jnp.where(mine, tags[:, i : i + 1, :], 0.0)
        own = own.reshape(n, LANES).astype(jnp.bfloat16)
        return jnp.dot(own, ones, preferred_element_type=f32)

    column = down(0) * DIGIT + down(1)
    deltas = got_ref[:, 0:cap, :].reshape(n, width)
    values = jnp.concatenate([deltas, jnp.ones((n, LANES), jnp.bfloat16)], axis=1)
    block = min(SLOT_BLOCK, n)
    for b in range(n // block):
        mark = jnp.concatenate([column[b * block : (b + 1) * block]] * (n // LANES), axis=1)
        weighted = jnp.where(mark == row_f, weight_row, 0.0).astype(jnp.bfloat16)
        sums[b * block : (b + 1) * block] = jnp.dot(weighted, values, preferred_element_type=f32)
    ids_copy.wait()
    sub = lax.broadcasted_iota(jnp.int32, (SUBLANES, width), 0)

    def rows_at(ref, ids):
        rows = jnp.broadcast_to(ref[pl.ds(ids[0], 1), :], (SUBLANES, width))
        for k in range(1, SUBLANES):
            row = jnp.broadcast_to(ref[pl.ds(ids[k], 1), :], (SUBLANES, width))
            rows = jnp.where(sub == k, row, rows)
        return rows

    def update(g):
        start = g * GROUP
        lane = start % LANES if isinstance(g, int) else lax.rem(start, LANES)
        fresh = []
        for half in range(GROUP // SUBLANES):
            at = half * SUBLANES
            ids = [id_smem[start // LANES, lane + at + k] for k in range(SUBLANES)]
            part = pl.ds(start + at, SUBLANES)
            grad = sums[part, 0:width] / jnp.maximum(sums[part, width : width + LANES], 1.0)
            next_a = rows_at(accum_ref, ids) + grad * grad
            next_t = rows_at(table_ref, ids) - learn_rate * grad / (jnp.sqrt(next_a) + epsilon)
            new_a_ref[part] = next_a
            new_t_ref[part] = next_t
            fresh.append(next_t)
        reply_ref[pl.ds(start, GROUP)] = jnp.concatenate(fresh, axis=0).astype(jnp.bfloat16)

    if n == block:
        for g in range(n // GROUP):
            update(g)
    else:

        def step(g, carry):
            update(g)
            return carry

        lax.fori_loop(0, n // GROUP, step, 0, unroll=2)


def write_kernel(
    ids_ref, new_t_ref, new_a_ref, table_hbm, accum_hbm, out_t, out_a,
    id_smem, tab, acc, sem_t, sem_a, sem_i,
):
    loads = copies(table_hbm, tab, sem_t) + copies(accum_hbm, acc, sem_a)
    for load in loads:
        load.start()
    ids_copy = pltpu.make_async_copy(ids_ref, id_smem, sem_i)
    ids_copy.start()
    ids_copy.wait()
    for load in loads:
        load.wait()

    def put(s, row, lane):
        v = id_smem[row, lane]
        tab[pl.ds(v, 1), :] = new_t_ref[pl.ds(s, 1), :]
        acc[pl.ds(v, 1), :] = new_a_ref[pl.ds(s, 1), :]

    each_slot(new_t_ref.shape[0], put)
    stores = copies(tab, out_t, sem_t) + copies(acc, out_a, sem_a)
    for store in stores:
        store.start()
    for store in stores:
        store.wait()


def in_hbm(*arrays):
    return [pltpu.with_memory_space_constraint(x, pltpu.HBM) for x in arrays]


def on_device(deltas, row_ids, sample_counts, live, table, accum):
    axes = ("aa", "ba")
    n_dest = lax.axis_size(axes)
    width = deltas.shape[1]
    n = deltas.shape[0]
    cap = n // n_dest
    vmem = pl.BlockSpec(memory_space=pltpu.VMEM)
    hbm = pl.BlockSpec(memory_space=pltpu.HBM)
    f32 = jnp.float32
    slots_vmem = 16 * MIB if n <= SLOT_BLOCK else 60 * MIB
    write_vmem = 16 * MIB
    payload = pl.pallas_call(
        functools.partial(pack_kernel, cap),
        out_shape=jax.ShapeDtypeStruct((n_dest, cap + TAG_ROWS, width), jnp.bfloat16),
        in_specs=[hbm] * 4,
        out_specs=vmem,
        scratch_shapes=[pltpu.VMEM((n,), jnp.int32)] * 3 + [pltpu.SemaphoreType.DMA((4,))],
        compiler_params=pltpu.CompilerParams(vmem_limit_bytes=PACK_VMEM),
        cost_estimate=pl.CostEstimate(flops=10**10, transcendentals=0, bytes_accessed=2**24),
        name="pack",
    )(*in_hbm(deltas.reshape(n_dest, cap, width), row_ids, sample_counts, live))
    got = lax.all_to_all(payload, axes, split_axis=0, concat_axis=0, tiled=True)
    rows = jax.ShapeDtypeStruct((n, width), f32)
    held = [pltpu.VMEM(table.shape, f32), pltpu.VMEM(accum.shape, f32)]
    replies, new_t, new_a, ids = pl.pallas_call(
        functools.partial(slots_kernel, cap, axes),
        out_shape=(
            jax.ShapeDtypeStruct((n, width), jnp.bfloat16), rows, rows,
            jax.ShapeDtypeStruct((n // LANES, LANES), jnp.int32),
        ),
        in_specs=[vmem] * 3,
        out_specs=(vmem,) * 4,
        scratch_shapes=[
            pltpu.SMEM((n // LANES, LANES), jnp.int32),
            pltpu.VMEM((n, width + LANES), f32), pltpu.SemaphoreType.DMA,
        ],
        compiler_params=pltpu.CompilerParams(vmem_limit_bytes=slots_vmem),
        name="slots",
    )(got, table, accum)
    returned = lax.all_to_all(
        replies.reshape(n_dest, cap, width), axes, split_axis=0, concat_axis=0, tiled=True
    )
    new_table, new_accum = pl.pallas_call(
        write_kernel,
        out_shape=(
            jax.ShapeDtypeStruct(table.shape, f32), jax.ShapeDtypeStruct(accum.shape, f32),
        ),
        in_specs=[vmem, vmem, vmem, hbm, hbm],
        out_specs=(hbm, hbm),
        scratch_shapes=[pltpu.SMEM((n // LANES, LANES), jnp.int32)] + held + [
            pltpu.SemaphoreType.DMA((COPIES,)), pltpu.SemaphoreType.DMA((COPIES,)),
            pltpu.SemaphoreType.DMA,
        ],
        cost_estimate=pl.CostEstimate(flops=10**9, transcendentals=0, bytes_accessed=8 * 2**20),
        compiler_params=pltpu.CompilerParams(vmem_limit_bytes=write_vmem),
        name="write",
    )(ids, new_t, new_a, *in_hbm(table, accum))
    return (new_table, new_accum, returned.reshape(-1, width))


def solution(mesh):
    placed = (
        P(("aa", "ba"), None),
        P(("aa", "ba")),
        P(("aa", "ba")),
        P(("aa", "ba")),
        P(("aa", "ba"), None),
        P(("aa", "ba"), None),
    )
    return jax.shard_map(
        on_device,
        mesh=mesh,
        in_specs=placed,
        out_specs=(P(("aa", "ba"), None), P(("aa", "ba"), None), P(("aa", "ba"), None)),
        check_vma=False,
    )
```

```python
import functools
import math

import jax
import jax.numpy as jnp
from jax import lax
from jax.experimental import pallas as pl
from jax.experimental.pallas import tpu as pltpu
from jax.sharding import PartitionSpec as P

learn_rate = 0.1
epsilon = 1e-08

LANES = 128
SUBLANES = 8
GROUP = 16
TAG_ROWS = 4
TILE = 4
DIGIT = 256
SLOT_BLOCK = 512
COPIES = 4
MIB = 2**20
PACK_VMEM = 8 * MIB


def as_rows(ref):
    n_dest, tiles, _, width = ref.shape
    return ref.reshape(n_dest * tiles * TILE, width)


def pack_kernel(
    cap, order, deltas_hbm, ids_hbm, counts_hbm, live_hbm, out_ref,
    deltas_ref, ids_ref, counts_ref, live_ref, sem, sem_d,
):
    per = LANES // cap
    n_dest = out_ref.shape[0]
    rows = cap + TAG_ROWS
    loads = [
        pltpu.make_async_copy(ids_hbm, ids_ref, sem.at[0]),
        pltpu.make_async_copy(counts_hbm, counts_ref, sem.at[1]),
        pltpu.make_async_copy(live_hbm, live_ref, sem.at[2]),
    ]
    loads_d = copies(deltas_hbm, deltas_ref, sem_d)
    for load in loads + loads_d:
        load.start()
    for load in loads:
        load.wait()
    out = as_rows(out_ref)
    sub = lax.broadcasted_iota(jnp.int32, (TAG_ROWS, LANES), 0)
    place = sorted(range(n_dest), key=order.__getitem__)
    for r in range(n_dest // per):
        lanes = pl.ds(r * LANES, LANES)
        ids = ids_ref[lanes][None, :]
        weight = (counts_ref[lanes] * live_ref[lanes])[None, :]
        upper = lax.shift_right_logical(ids, 8)
        lower = jnp.bitwise_and(ids, DIGIT - 1)
        tag = jnp.where(sub == 0, upper, jnp.where(sub == 1, lower, jnp.where(sub == 2, weight, 0)))
        tag = tag.astype(jnp.float32).astype(jnp.bfloat16)
        for owner in range(r * per, (r + 1) * per):
            k = place[owner]
            out[k * rows + cap : (k + 1) * rows] = tag
    for load in loads_d:
        load.wait()
    for k in range(n_dest):
        owner = order[k]
        out[k * rows : k * rows + cap] = deltas_ref[owner * cap : (owner + 1) * cap]


def copies(src, dst, sem):
    rows = src.shape[0] // COPIES
    return [
        pltpu.make_async_copy(
            src.at[pl.ds(i * rows, rows)], dst.at[pl.ds(i * rows, rows)], sem.at[i]
        )
        for i in range(COPIES)
    ]


def gather_ids(cap, axes, got_ref, id_rows, id_smem, sem):
    n_src = got_ref.shape[0]
    got = as_rows(got_ref)
    rows = cap + TAG_ROWS
    per = LANES // cap
    mine = lax.rem(lax.axis_index(axes), per)
    lane = lax.broadcasted_iota(jnp.int32, (TAG_ROWS, LANES), 1)
    own = lane // cap == mine
    ids, weights = [], []
    for r in range(n_src // per):
        tile = jnp.zeros((TAG_ROWS, LANES), jnp.float32)
        for k in range(per):
            p = r * per + k
            tag = got[p * rows + cap : (p + 1) * rows].astype(jnp.float32)
            shift = lax.rem(k - mine + per, per) * cap
            tile = tile + pltpu.roll(jnp.where(own, tag, 0.0), shift, 1)
        row = tile[0:1] * DIGIT + tile[1:2]
        id_rows[r : r + 1] = row.astype(jnp.int32)
        ids.append(row)
        weights.append(tile[2:3])
    copy = pltpu.make_async_copy(id_rows, id_smem, sem)
    copy.start()
    return jnp.concatenate(ids, axis=1), jnp.concatenate(weights, axis=1), copy


def each_slot(n, body):
    block = min(SLOT_BLOCK, n)

    def one_block(b):
        for k in range(block):
            s = b * block + k
            body(s, s // LANES, s % LANES)

    if n == block:
        one_block(0)
    else:

        def step(s, carry):
            body(s, s // LANES, lax.rem(s, LANES))
            return carry

        lax.fori_loop(0, n, step, 0, unroll=32)


def slots_kernel(
    cap, axes, got_ref, table_ref, accum_ref, reply_ref, new_t_ref, new_a_ref, ids_ref,
    id_smem, sums, sem_i,
):
    n_src, _, _, width = got_ref.shape
    n = n_src * cap
    got = as_rows(got_ref)
    rows = cap + TAG_ROWS
    row_f, weight_row, ids_copy = gather_ids(cap, axes, got_ref, ids_ref, id_smem, sem_i)
    per = LANES // cap
    first = lax.rem(lax.axis_index(axes), per) * cap
    lane = lax.broadcasted_iota(jnp.int32, (cap, LANES), 1)
    slot = lax.broadcasted_iota(jnp.int32, (cap, LANES), 0)
    mine = lane == slot + first
    tags = [got[p * rows + cap : (p + 1) * rows].astype(jnp.float32) for p in range(n_src)]
    ones = jnp.ones((LANES, LANES), jnp.bfloat16)
    f32 = jnp.float32

    def down(i):
        own = [jnp.where(mine, tag[i : i + 1], 0.0).astype(jnp.bfloat16) for tag in tags]
        return jnp.dot(jnp.concatenate(own, axis=0), ones, preferred_element_type=f32)

    column = down(0) * DIGIT + down(1)
    deltas = [got[p * rows : p * rows + cap] for p in range(n_src)]
    deltas = jnp.concatenate(deltas, axis=0)
    values = jnp.concatenate([deltas, jnp.ones((n, LANES), jnp.bfloat16)], axis=1)
    block = min(SLOT_BLOCK, n)
    for b in range(n // block):
        mark = jnp.concatenate([column[b * block : (b + 1) * block]] * (n // LANES), axis=1)
        weighted = jnp.where(mark == row_f, weight_row, 0.0).astype(jnp.bfloat16)
        sums[b * block : (b + 1) * block] = jnp.dot(weighted, values, preferred_element_type=f32)
    ids_copy.wait()
    sub = lax.broadcasted_iota(jnp.int32, (SUBLANES, width), 0)

    def rows_at(ref, ids):
        rows = jnp.broadcast_to(ref[pl.ds(ids[0], 1), :], (SUBLANES, width))
        for k in range(1, SUBLANES):
            row = jnp.broadcast_to(ref[pl.ds(ids[k], 1), :], (SUBLANES, width))
            rows = jnp.where(sub == k, row, rows)
        return rows

    def update(g):
        start = g * GROUP
        lane = start % LANES if isinstance(g, int) else lax.rem(start, LANES)
        fresh = []
        for half in range(GROUP // SUBLANES):
            at = half * SUBLANES
            ids = [id_smem[start // LANES, lane + at + k] for k in range(SUBLANES)]
            part = pl.ds(start + at, SUBLANES)
            grad = sums[part, 0:width] / jnp.maximum(sums[part, width : width + LANES], 1.0)
            next_a = rows_at(accum_ref, ids) + grad * grad
            next_t = rows_at(table_ref, ids) - learn_rate * grad / (jnp.sqrt(next_a) + epsilon)
            new_a_ref[part] = next_a
            new_t_ref[part] = next_t
            fresh.append(next_t)
        reply_ref[pl.ds(start, GROUP)] = jnp.concatenate(fresh, axis=0).astype(jnp.bfloat16)

    if n == block:
        for g in range(n // GROUP):
            update(g)
    else:

        def step(g, carry):
            update(g)
            return carry

        lax.fori_loop(0, n // GROUP, step, 0, unroll=2)


def write_kernel(
    ids_ref, new_t_ref, new_a_ref, table_hbm, accum_hbm, out_t, out_a,
    id_smem, tab, acc, sem_t, sem_a, sem_i,
):
    loads = copies(table_hbm, tab, sem_t) + copies(accum_hbm, acc, sem_a)
    for load in loads:
        load.start()
    ids_copy = pltpu.make_async_copy(ids_ref, id_smem, sem_i)
    ids_copy.start()
    ids_copy.wait()
    for load in loads:
        load.wait()

    def put(s, row, lane):
        v = id_smem[row, lane]
        tab[pl.ds(v, 1), :] = new_t_ref[pl.ds(s, 1), :]
        acc[pl.ds(v, 1), :] = new_a_ref[pl.ds(s, 1), :]

    each_slot(new_t_ref.shape[0], put)
    stores = copies(tab, out_t, sem_t) + copies(acc, out_a, sem_a)
    for store in stores:
        store.start()
    for store in stores:
        store.wait()


def finish_kernel(cap, order, returned_ref, fresh_ref):
    for k, owner in enumerate(order):
        fresh_ref[owner * cap : (owner + 1) * cap] = returned_ref[k * cap : (k + 1) * cap]


def block_order(n_dest):
    step = -5 if math.gcd(n_dest, 5) == 1 else -1
    return [step * k % n_dest for k in range(n_dest)]


def exchange(blocks, axes, order):
    return lax.all_to_all(
        blocks, axes, split_axis=0, concat_axis=0, tiled=True, axis_index_groups=[order]
    )


def in_hbm(*arrays):
    return [pltpu.with_memory_space_constraint(x, pltpu.HBM) for x in arrays]


def on_device(deltas, row_ids, sample_counts, live, table, accum):
    axes = ("aa", "ba")
    n_dest = lax.axis_size(axes)
    width = deltas.shape[1]
    n = deltas.shape[0]
    cap = n // n_dest
    order = block_order(n_dest)
    vmem = pl.BlockSpec(memory_space=pltpu.VMEM)
    hbm = pl.BlockSpec(memory_space=pltpu.HBM)
    f32 = jnp.float32
    slots_vmem = 16 * MIB if n <= SLOT_BLOCK else 60 * MIB
    write_vmem = 16 * MIB
    payload = pl.pallas_call(
        functools.partial(pack_kernel, cap, order),
        out_shape=jax.ShapeDtypeStruct(
            (n_dest, (cap + TAG_ROWS) // TILE, TILE, width), jnp.bfloat16
        ),
        in_specs=[hbm] * 4,
        out_specs=vmem,
        scratch_shapes=[pltpu.VMEM((n, width), jnp.bfloat16)]
        + [pltpu.VMEM((n,), jnp.int32)] * 3
        + [pltpu.SemaphoreType.DMA((3,)), pltpu.SemaphoreType.DMA((COPIES,))],
        compiler_params=pltpu.CompilerParams(vmem_limit_bytes=PACK_VMEM),
        cost_estimate=pl.CostEstimate(flops=10**10, transcendentals=0, bytes_accessed=2**24),
        name="pack",
    )(*in_hbm(deltas, row_ids, sample_counts, live))
    got = exchange(payload, axes, order)
    rows = jax.ShapeDtypeStruct((n, width), f32)
    held = [pltpu.VMEM(table.shape, f32), pltpu.VMEM(accum.shape, f32)]
    replies, new_t, new_a, ids = pl.pallas_call(
        functools.partial(slots_kernel, cap, axes),
        out_shape=(
            jax.ShapeDtypeStruct((n, width), jnp.bfloat16), rows, rows,
            jax.ShapeDtypeStruct((n // LANES, LANES), jnp.int32),
        ),
        in_specs=[vmem] * 3,
        out_specs=(vmem,) * 4,
        scratch_shapes=[
            pltpu.SMEM((n // LANES, LANES), jnp.int32),
            pltpu.VMEM((n, width + LANES), f32), pltpu.SemaphoreType.DMA,
        ],
        compiler_params=pltpu.CompilerParams(vmem_limit_bytes=slots_vmem),
        name="slots",
    )(got, table, accum)
    returned = exchange(replies.reshape(n_dest, cap, width), axes, order)
    new_table, new_accum = pl.pallas_call(
        write_kernel,
        out_shape=(
            jax.ShapeDtypeStruct(table.shape, f32), jax.ShapeDtypeStruct(accum.shape, f32),
        ),
        in_specs=[vmem, vmem, vmem, hbm, hbm],
        out_specs=(hbm, hbm),
        scratch_shapes=[pltpu.SMEM((n // LANES, LANES), jnp.int32)] + held + [
            pltpu.SemaphoreType.DMA((COPIES,)), pltpu.SemaphoreType.DMA((COPIES,)),
            pltpu.SemaphoreType.DMA,
        ],
        cost_estimate=pl.CostEstimate(flops=10**9, transcendentals=0, bytes_accessed=8 * 2**20),
        compiler_params=pltpu.CompilerParams(vmem_limit_bytes=write_vmem),
        name="write",
    )(ids, new_t, new_a, *in_hbm(table, accum))
    fresh = pl.pallas_call(
        functools.partial(finish_kernel, cap, order),
        out_shape=jax.ShapeDtypeStruct((n, width), jnp.bfloat16),
        in_specs=[vmem],
        out_specs=vmem,
        compiler_params=pltpu.CompilerParams(vmem_limit_bytes=PACK_VMEM),
        name="finish",
    )(returned.reshape(-1, width))
    return (new_table, new_accum, fresh)


def solution(mesh):
    placed = (
        P(("aa", "ba"), None),
        P(("aa", "ba")),
        P(("aa", "ba")),
        P(("aa", "ba")),
        P(("aa", "ba"), None),
        P(("aa", "ba"), None),
    )
    return jax.shard_map(
        on_device,
        mesh=mesh,
        in_specs=placed,
        out_specs=(P(("aa", "ba"), None), P(("aa", "ba"), None), P(("aa", "ba"), None)),
        check_vma=False,
    )
```

```python
import functools
import math

import jax
import jax.numpy as jnp
from jax import lax
from jax.experimental import pallas as pl
from jax.experimental.pallas import tpu as pltpu
from jax.sharding import PartitionSpec as P

learn_rate = 0.1
epsilon = 1e-08

LANES = 128
SUBLANES = 8
GROUP = 16
TAG_ROWS = 4
TILE = 4
DIGIT = 256
SLOT_BLOCK = 512
COPIES = 4
MIB = 2**20
PACK_VMEM = 8 * MIB


def as_rows(ref):
    n_dest, tiles, _, width = ref.shape
    return ref.reshape(n_dest * tiles * TILE, width)


def pack_kernel(
    cap, order, deltas_hbm, ids_hbm, counts_hbm, live_hbm, out_ref,
    deltas_ref, ids_ref, counts_ref, live_ref, sem, sem_d,
):
    per = LANES // cap
    n_dest = out_ref.shape[0]
    rows = cap + TAG_ROWS
    loads = [
        pltpu.make_async_copy(ids_hbm, ids_ref, sem.at[0]),
        pltpu.make_async_copy(counts_hbm, counts_ref, sem.at[1]),
        pltpu.make_async_copy(live_hbm, live_ref, sem.at[2]),
    ]
    loads_d = copies(deltas_hbm, deltas_ref, sem_d)
    for load in loads + loads_d:
        load.start()
    for load in loads:
        load.wait()
    out = as_rows(out_ref)
    sub = lax.broadcasted_iota(jnp.int32, (TAG_ROWS, LANES), 0)
    place = sorted(range(n_dest), key=order.__getitem__)
    for r in range(n_dest // per):
        lanes = pl.ds(r * LANES, LANES)
        ids = ids_ref[lanes][None, :]
        weight = (counts_ref[lanes] * live_ref[lanes])[None, :]
        upper = lax.shift_right_logical(ids, 8)
        lower = jnp.bitwise_and(ids, DIGIT - 1)
        tag = jnp.where(sub == 0, upper, jnp.where(sub == 1, lower, jnp.where(sub == 2, weight, 0)))
        tag = tag.astype(jnp.float32).astype(jnp.bfloat16)
        for owner in range(r * per, (r + 1) * per):
            k = place[owner]
            out[k * rows + cap : (k + 1) * rows] = tag
    for load in loads_d:
        load.wait()
    for k in range(n_dest):
        owner = order[k]
        out[k * rows : k * rows + cap] = deltas_ref[owner * cap : (owner + 1) * cap]


def copies(src, dst, sem):
    rows = src.shape[0] // COPIES
    return [
        pltpu.make_async_copy(
            src.at[pl.ds(i * rows, rows)], dst.at[pl.ds(i * rows, rows)], sem.at[i]
        )
        for i in range(COPIES)
    ]


def gather_ids(cap, axes, got_ref, id_rows, id_smem, sem):
    n_src = got_ref.shape[0]
    got = as_rows(got_ref)
    rows = cap + TAG_ROWS
    per = LANES // cap
    mine = lax.rem(lax.axis_index(axes), per)
    lane = lax.broadcasted_iota(jnp.int32, (TAG_ROWS, LANES), 1)
    own = lane // cap == mine
    ids, weights = [], []
    for r in range(n_src // per):
        tile = jnp.zeros((TAG_ROWS, LANES), jnp.float32)
        for k in range(per):
            p = r * per + k
            tag = got[p * rows + cap : (p + 1) * rows].astype(jnp.float32)
            shift = lax.rem(k - mine + per, per) * cap
            tile = tile + pltpu.roll(jnp.where(own, tag, 0.0), shift, 1)
        row = tile[0:1] * DIGIT + tile[1:2]
        id_rows[r : r + 1] = row.astype(jnp.int32)
        ids.append(row)
        weights.append(tile[2:3])
    copy = pltpu.make_async_copy(id_rows, id_smem, sem)
    copy.start()
    return jnp.concatenate(ids, axis=1), jnp.concatenate(weights, axis=1), copy


def each_slot(n, body):
    block = min(SLOT_BLOCK, n)

    def one_block(b):
        for k in range(block):
            s = b * block + k
            body(s, s // LANES, s % LANES)

    if n == block:
        one_block(0)
    else:

        def step(s, carry):
            body(s, s // LANES, lax.rem(s, LANES))
            return carry

        lax.fori_loop(0, n, step, 0, unroll=32)


def slots_kernel(
    cap, axes, got_ref, table_ref, accum_ref, reply_ref, new_t_ref, new_a_ref, ids_ref,
    id_smem, sums, sem_i,
):
    n_src, _, _, width = got_ref.shape
    n = n_src * cap
    got = as_rows(got_ref)
    rows = cap + TAG_ROWS
    row_f, weight_row, ids_copy = gather_ids(cap, axes, got_ref, ids_ref, id_smem, sem_i)
    per = LANES // cap
    first = lax.rem(lax.axis_index(axes), per) * cap
    lane = lax.broadcasted_iota(jnp.int32, (cap, LANES), 1)
    slot = lax.broadcasted_iota(jnp.int32, (cap, LANES), 0)
    mine = lane == slot + first
    tags = [got[p * rows + cap : (p + 1) * rows].astype(jnp.float32) for p in range(n_src)]
    ones = jnp.ones((LANES, LANES), jnp.bfloat16)
    f32 = jnp.float32

    def down(i):
        own = [jnp.where(mine, tag[i : i + 1], 0.0).astype(jnp.bfloat16) for tag in tags]
        return jnp.dot(jnp.concatenate(own, axis=0), ones, preferred_element_type=f32)

    column = down(0) * DIGIT + down(1)
    deltas = [got[p * rows : p * rows + cap] for p in range(n_src)]
    deltas = jnp.concatenate(deltas, axis=0)
    values = jnp.concatenate([deltas, jnp.ones((n, LANES), jnp.bfloat16)], axis=1)
    block = min(SLOT_BLOCK, n)
    for b in range(n // block):
        mark = jnp.concatenate([column[b * block : (b + 1) * block]] * (n // LANES), axis=1)
        weighted = jnp.where(mark == row_f, weight_row, 0.0).astype(jnp.bfloat16)
        sums[b * block : (b + 1) * block] = jnp.dot(weighted, values, preferred_element_type=f32)
    ids_copy.wait()
    sub = lax.broadcasted_iota(jnp.int32, (SUBLANES, width), 0)

    def rows_at(ref, ids):
        rows = jnp.broadcast_to(ref[pl.ds(ids[0], 1), :], (SUBLANES, width))
        for k in range(1, SUBLANES):
            row = jnp.broadcast_to(ref[pl.ds(ids[k], 1), :], (SUBLANES, width))
            rows = jnp.where(sub == k, row, rows)
        return rows

    def update(g):
        start = g * GROUP
        lane = start % LANES if isinstance(g, int) else lax.rem(start, LANES)
        fresh = []
        for half in range(GROUP // SUBLANES):
            at = half * SUBLANES
            ids = [id_smem[start // LANES, lane + at + k] for k in range(SUBLANES)]
            part = pl.ds(start + at, SUBLANES)
            grad = sums[part, 0:width] / jnp.maximum(sums[part, width : width + LANES], 1.0)
            next_a = rows_at(accum_ref, ids) + grad * grad
            next_t = rows_at(table_ref, ids) - learn_rate * grad / (jnp.sqrt(next_a) + epsilon)
            new_a_ref[part] = next_a
            new_t_ref[part] = next_t
            fresh.append(next_t)
        reply_ref[pl.ds(start, GROUP)] = jnp.concatenate(fresh, axis=0).astype(jnp.bfloat16)

    if n == block:
        for g in range(n // GROUP):
            update(g)
    else:

        def step(g, carry):
            update(g)
            return carry

        lax.fori_loop(0, n // GROUP, step, 0, unroll=2)


def write_kernel(
    ids_ref, new_t_ref, new_a_ref, table_hbm, accum_hbm, out_t, out_a,
    id_smem, tab, acc, sem_t, sem_a, sem_i,
):
    loads = copies(table_hbm, tab, sem_t) + copies(accum_hbm, acc, sem_a)
    for load in loads:
        load.start()
    ids_copy = pltpu.make_async_copy(ids_ref, id_smem, sem_i)
    ids_copy.start()
    ids_copy.wait()
    for load in loads:
        load.wait()

    def put(s, row, lane):
        v = id_smem[row, lane]
        tab[pl.ds(v, 1), :] = new_t_ref[pl.ds(s, 1), :]
        acc[pl.ds(v, 1), :] = new_a_ref[pl.ds(s, 1), :]

    each_slot(new_t_ref.shape[0], put)
    stores = copies(tab, out_t, sem_t) + copies(acc, out_a, sem_a)
    for store in stores:
        store.start()
    for store in stores:
        store.wait()


def finish_kernel(cap, order, returned_ref, fresh_ref):
    for k, owner in enumerate(order):
        fresh_ref[owner * cap : (owner + 1) * cap] = returned_ref[k * cap : (k + 1) * cap]


def block_order(n_first, n_second):
    n_dest = n_first * n_second
    order = [
        (3 * k - k // n_second) % n_first * n_second + 3 * k % n_second for k in range(n_dest)
    ]
    return order if len(set(order)) == n_dest else list(range(n_dest))


def exchange(blocks, axes, order):
    return lax.all_to_all(
        blocks, axes, split_axis=0, concat_axis=0, tiled=True, axis_index_groups=[order]
    )


def in_hbm(*arrays):
    return [pltpu.with_memory_space_constraint(x, pltpu.HBM) for x in arrays]


def on_device(deltas, row_ids, sample_counts, live, table, accum):
    axes = ("aa", "ba")
    n_dest = lax.axis_size(axes)
    width = deltas.shape[1]
    n = deltas.shape[0]
    cap = n // n_dest
    order = block_order(*(lax.axis_size(axis) for axis in axes))
    vmem = pl.BlockSpec(memory_space=pltpu.VMEM)
    hbm = pl.BlockSpec(memory_space=pltpu.HBM)
    f32 = jnp.float32
    slots_vmem = 16 * MIB if n <= SLOT_BLOCK else 60 * MIB
    write_vmem = 16 * MIB
    payload = pl.pallas_call(
        functools.partial(pack_kernel, cap, order),
        out_shape=jax.ShapeDtypeStruct(
            (n_dest, (cap + TAG_ROWS) // TILE, TILE, width), jnp.bfloat16
        ),
        in_specs=[hbm] * 4,
        out_specs=vmem,
        scratch_shapes=[pltpu.VMEM((n, width), jnp.bfloat16)]
        + [pltpu.VMEM((n,), jnp.int32)] * 3
        + [pltpu.SemaphoreType.DMA((3,)), pltpu.SemaphoreType.DMA((COPIES,))],
        compiler_params=pltpu.CompilerParams(vmem_limit_bytes=PACK_VMEM),
        cost_estimate=pl.CostEstimate(flops=10**10, transcendentals=0, bytes_accessed=2**24),
        name="pack",
    )(*in_hbm(deltas, row_ids, sample_counts, live))
    got = exchange(payload, axes, order)
    rows = jax.ShapeDtypeStruct((n, width), f32)
    held = [pltpu.VMEM(table.shape, f32), pltpu.VMEM(accum.shape, f32)]
    replies, new_t, new_a, ids = pl.pallas_call(
        functools.partial(slots_kernel, cap, axes),
        out_shape=(
            jax.ShapeDtypeStruct((n, width), jnp.bfloat16), rows, rows,
            jax.ShapeDtypeStruct((n // LANES, LANES), jnp.int32),
        ),
        in_specs=[vmem] * 3,
        out_specs=(vmem,) * 4,
        scratch_shapes=[
            pltpu.SMEM((n // LANES, LANES), jnp.int32),
            pltpu.VMEM((n, width + LANES), f32), pltpu.SemaphoreType.DMA,
        ],
        compiler_params=pltpu.CompilerParams(vmem_limit_bytes=slots_vmem),
        name="slots",
    )(got, table, accum)
    returned = exchange(replies.reshape(n_dest, cap, width), axes, order)
    new_table, new_accum = pl.pallas_call(
        write_kernel,
        out_shape=(
            jax.ShapeDtypeStruct(table.shape, f32), jax.ShapeDtypeStruct(accum.shape, f32),
        ),
        in_specs=[vmem, vmem, vmem, hbm, hbm],
        out_specs=(hbm, hbm),
        scratch_shapes=[pltpu.SMEM((n // LANES, LANES), jnp.int32)] + held + [
            pltpu.SemaphoreType.DMA((COPIES,)), pltpu.SemaphoreType.DMA((COPIES,)),
            pltpu.SemaphoreType.DMA,
        ],
        cost_estimate=pl.CostEstimate(flops=10**9, transcendentals=0, bytes_accessed=8 * 2**20),
        compiler_params=pltpu.CompilerParams(vmem_limit_bytes=write_vmem),
        name="write",
    )(ids, new_t, new_a, *in_hbm(table, accum))
    fresh = pl.pallas_call(
        functools.partial(finish_kernel, cap, order),
        out_shape=jax.ShapeDtypeStruct((n, width), jnp.bfloat16),
        in_specs=[vmem],
        out_specs=vmem,
        compiler_params=pltpu.CompilerParams(vmem_limit_bytes=PACK_VMEM),
        name="finish",
    )(returned.reshape(-1, width))
    return (new_table, new_accum, fresh)


def solution(mesh):
    placed = (
        P(("aa", "ba"), None),
        P(("aa", "ba")),
        P(("aa", "ba")),
        P(("aa", "ba")),
        P(("aa", "ba"), None),
        P(("aa", "ba"), None),
    )
    return jax.shard_map(
        on_device,
        mesh=mesh,
        in_specs=placed,
        out_specs=(P(("aa", "ba"), None), P(("aa", "ba"), None), P(("aa", "ba"), None)),
        check_vma=False,
    )
```

```python
import functools
import math

import jax
import jax.numpy as jnp
from jax import lax
from jax.experimental import pallas as pl
from jax.experimental.pallas import tpu as pltpu
from jax.sharding import PartitionSpec as P

learn_rate = 0.1
epsilon = 1e-08

LANES = 128
SUBLANES = 8
GROUP = 16
TAG_ROWS = 4
TILE = 4
DIGIT = 256
SLOT_BLOCK = 512
COPIES = 4
MIB = 2**20
PACK_VMEM = 8 * MIB


def as_rows(ref):
    n_dest, tiles, _, width = ref.shape
    return ref.reshape(n_dest * tiles * TILE, width)


def pack_kernel(
    cap, order, deltas_hbm, ids_hbm, counts_hbm, live_hbm, out_ref,
    deltas_ref, ids_ref, counts_ref, live_ref, sem, sem_d,
):
    per = LANES // cap
    n_dest = out_ref.shape[0]
    rows = cap + TAG_ROWS
    loads = [
        pltpu.make_async_copy(ids_hbm, ids_ref, sem.at[0]),
        pltpu.make_async_copy(counts_hbm, counts_ref, sem.at[1]),
        pltpu.make_async_copy(live_hbm, live_ref, sem.at[2]),
    ]
    loads_d = copies(deltas_hbm, deltas_ref, sem_d)
    for load in loads_d + loads:
        load.start()
    for load in loads:
        load.wait()
    out = as_rows(out_ref)
    sub = lax.broadcasted_iota(jnp.int32, (TAG_ROWS, LANES), 0)
    place = sorted(range(n_dest), key=order.__getitem__)
    for r in range(n_dest // per):
        lanes = pl.ds(r * LANES, LANES)
        ids = ids_ref[lanes][None, :]
        weight = (counts_ref[lanes] * live_ref[lanes])[None, :]
        upper = lax.shift_right_logical(ids, 8)
        lower = jnp.bitwise_and(ids, DIGIT - 1)
        tag = jnp.where(sub == 0, upper, jnp.where(sub == 1, lower, jnp.where(sub == 2, weight, 0)))
        tag = tag.astype(jnp.float32).astype(jnp.bfloat16)
        for owner in range(r * per, (r + 1) * per):
            k = place[owner]
            out[k * rows + cap : (k + 1) * rows] = tag
    part = n_dest // COPIES
    for owner in range(n_dest):
        if owner % part == 0:
            loads_d[owner // part].wait()
        k = place[owner]
        out[k * rows : k * rows + cap] = deltas_ref[owner * cap : (owner + 1) * cap]


def copies(src, dst, sem):
    rows = src.shape[0] // COPIES
    return [
        pltpu.make_async_copy(
            src.at[pl.ds(i * rows, rows)], dst.at[pl.ds(i * rows, rows)], sem.at[i]
        )
        for i in range(COPIES)
    ]


def gather_ids(cap, axes, got_ref, id_rows, id_smem, sem):
    n_src = got_ref.shape[0]
    got = as_rows(got_ref)
    rows = cap + TAG_ROWS
    per = LANES // cap
    mine = lax.rem(lax.axis_index(axes), per)
    lane = lax.broadcasted_iota(jnp.int32, (TAG_ROWS, LANES), 1)
    own = lane // cap == mine
    ids, weights = [], []
    for r in range(n_src // per):
        tile = jnp.zeros((TAG_ROWS, LANES), jnp.float32)
        for k in range(per):
            p = r * per + k
            tag = got[p * rows + cap : (p + 1) * rows].astype(jnp.float32)
            shift = lax.rem(k - mine + per, per) * cap
            tile = tile + pltpu.roll(jnp.where(own, tag, 0.0), shift, 1)
        row = tile[0:1] * DIGIT + tile[1:2]
        id_rows[r : r + 1] = row.astype(jnp.int32)
        ids.append(row)
        weights.append(tile[2:3])
    copy = pltpu.make_async_copy(id_rows, id_smem, sem)
    copy.start()
    return jnp.concatenate(ids, axis=1), jnp.concatenate(weights, axis=1), copy


def each_slot(n, body):
    block = min(SLOT_BLOCK, n)

    def one_block(b):
        for k in range(block):
            s = b * block + k
            body(s, s // LANES, s % LANES)

    if n == block:
        one_block(0)
    else:

        def step(s, carry):
            body(s, s // LANES, lax.rem(s, LANES))
            return carry

        lax.fori_loop(0, n, step, 0, unroll=32)


def slots_kernel(
    cap, axes, got_ref, table_ref, accum_ref, reply_ref, new_t_ref, new_a_ref, ids_ref,
    id_smem, sums, sem_i,
):
    n_src, _, _, width = got_ref.shape
    n = n_src * cap
    got = as_rows(got_ref)
    rows = cap + TAG_ROWS
    row_f, weight_row, ids_copy = gather_ids(cap, axes, got_ref, ids_ref, id_smem, sem_i)
    per = LANES // cap
    first = lax.rem(lax.axis_index(axes), per) * cap
    lane = lax.broadcasted_iota(jnp.int32, (cap, LANES), 1)
    slot = lax.broadcasted_iota(jnp.int32, (cap, LANES), 0)
    mine = lane == slot + first
    tags = [got[p * rows + cap : (p + 1) * rows].astype(jnp.float32) for p in range(n_src)]
    ones = jnp.ones((LANES, LANES), jnp.bfloat16)
    f32 = jnp.float32

    def down(i):
        own = [jnp.where(mine, tag[i : i + 1], 0.0).astype(jnp.bfloat16) for tag in tags]
        return jnp.dot(jnp.concatenate(own, axis=0), ones, preferred_element_type=f32)

    column = down(0) * DIGIT + down(1)
    deltas = [got[p * rows : p * rows + cap] for p in range(n_src)]
    deltas = jnp.concatenate(deltas, axis=0)
    values = jnp.concatenate([deltas, jnp.ones((n, LANES), jnp.bfloat16)], axis=1)
    block = min(SLOT_BLOCK, n)
    for b in range(n // block):
        mark = jnp.concatenate([column[b * block : (b + 1) * block]] * (n // LANES), axis=1)
        weighted = jnp.where(mark == row_f, weight_row, 0.0).astype(jnp.bfloat16)
        sums[b * block : (b + 1) * block] = jnp.dot(weighted, values, preferred_element_type=f32)
    ids_copy.wait()
    sub = lax.broadcasted_iota(jnp.int32, (SUBLANES, width), 0)

    def rows_at(ref, ids):
        rows = jnp.broadcast_to(ref[pl.ds(ids[0], 1), :], (SUBLANES, width))
        for k in range(1, SUBLANES):
            row = jnp.broadcast_to(ref[pl.ds(ids[k], 1), :], (SUBLANES, width))
            rows = jnp.where(sub == k, row, rows)
        return rows

    def update(g):
        start = g * GROUP
        lane = start % LANES if isinstance(g, int) else lax.rem(start, LANES)
        fresh = []
        for half in range(GROUP // SUBLANES):
            at = half * SUBLANES
            ids = [id_smem[start // LANES, lane + at + k] for k in range(SUBLANES)]
            part = pl.ds(start + at, SUBLANES)
            grad = sums[part, 0:width] / jnp.maximum(sums[part, width : width + LANES], 1.0)
            next_a = rows_at(accum_ref, ids) + grad * grad
            next_t = rows_at(table_ref, ids) - learn_rate * grad / (jnp.sqrt(next_a) + epsilon)
            new_a_ref[part] = next_a
            new_t_ref[part] = next_t
            fresh.append(next_t)
        reply_ref[pl.ds(start, GROUP)] = jnp.concatenate(fresh, axis=0).astype(jnp.bfloat16)

    if n == block:
        for g in range(n // GROUP):
            update(g)
    else:

        def step(g, carry):
            update(g)
            return carry

        lax.fori_loop(0, n // GROUP, step, 0, unroll=2)


def write_kernel(
    ids_ref, new_t_ref, new_a_ref, table_hbm, accum_hbm, out_t, out_a,
    id_smem, tab, acc, sem_t, sem_a, sem_i,
):
    loads = copies(table_hbm, tab, sem_t) + copies(accum_hbm, acc, sem_a)
    for load in loads:
        load.start()
    ids_copy = pltpu.make_async_copy(ids_ref, id_smem, sem_i)
    ids_copy.start()
    ids_copy.wait()
    for load in loads:
        load.wait()

    def put(s, row, lane):
        v = id_smem[row, lane]
        tab[pl.ds(v, 1), :] = new_t_ref[pl.ds(s, 1), :]
        acc[pl.ds(v, 1), :] = new_a_ref[pl.ds(s, 1), :]

    each_slot(new_t_ref.shape[0], put)
    stores = copies(tab, out_t, sem_t) + copies(acc, out_a, sem_a)
    for store in stores:
        store.start()
    for store in stores:
        store.wait()


def finish_kernel(cap, order, returned_ref, fresh_ref):
    for k, owner in enumerate(order):
        fresh_ref[owner * cap : (owner + 1) * cap] = returned_ref[k * cap : (k + 1) * cap]


def block_order(n_first, n_second):
    n_dest = n_first * n_second
    order = [
        (3 * k - k // n_second) % n_first * n_second + 3 * k % n_second for k in range(n_dest)
    ]
    return order if len(set(order)) == n_dest else list(range(n_dest))


def exchange(blocks, axes, order):
    return lax.all_to_all(
        blocks, axes, split_axis=0, concat_axis=0, tiled=True, axis_index_groups=[order]
    )


def in_hbm(*arrays):
    return [pltpu.with_memory_space_constraint(x, pltpu.HBM) for x in arrays]


def on_device(deltas, row_ids, sample_counts, live, table, accum):
    axes = ("aa", "ba")
    n_dest = lax.axis_size(axes)
    width = deltas.shape[1]
    n = deltas.shape[0]
    cap = n // n_dest
    order = block_order(*(lax.axis_size(axis) for axis in axes))
    vmem = pl.BlockSpec(memory_space=pltpu.VMEM)
    hbm = pl.BlockSpec(memory_space=pltpu.HBM)
    f32 = jnp.float32
    slots_vmem = 16 * MIB if n <= SLOT_BLOCK else 60 * MIB
    write_vmem = 16 * MIB
    payload = pl.pallas_call(
        functools.partial(pack_kernel, cap, order),
        out_shape=jax.ShapeDtypeStruct(
            (n_dest, (cap + TAG_ROWS) // TILE, TILE, width), jnp.bfloat16
        ),
        in_specs=[hbm] * 4,
        out_specs=vmem,
        scratch_shapes=[pltpu.VMEM((n, width), jnp.bfloat16)]
        + [pltpu.VMEM((n,), jnp.int32)] * 3
        + [pltpu.SemaphoreType.DMA((3,)), pltpu.SemaphoreType.DMA((COPIES,))],
        compiler_params=pltpu.CompilerParams(vmem_limit_bytes=PACK_VMEM),
        cost_estimate=pl.CostEstimate(flops=10**10, transcendentals=0, bytes_accessed=2**24),
        name="pack",
    )(*in_hbm(deltas, row_ids, sample_counts, live))
    got = exchange(payload, axes, order)
    rows = jax.ShapeDtypeStruct((n, width), f32)
    held = [pltpu.VMEM(table.shape, f32), pltpu.VMEM(accum.shape, f32)]
    replies, new_t, new_a, ids = pl.pallas_call(
        functools.partial(slots_kernel, cap, axes),
        out_shape=(
            jax.ShapeDtypeStruct((n, width), jnp.bfloat16), rows, rows,
            jax.ShapeDtypeStruct((n // LANES, LANES), jnp.int32),
        ),
        in_specs=[vmem] * 3,
        out_specs=(vmem,) * 4,
        scratch_shapes=[
            pltpu.SMEM((n // LANES, LANES), jnp.int32),
            pltpu.VMEM((n, width + LANES), f32), pltpu.SemaphoreType.DMA,
        ],
        compiler_params=pltpu.CompilerParams(vmem_limit_bytes=slots_vmem),
        name="slots",
    )(got, table, accum)
    returned = exchange(replies.reshape(n_dest, cap, width), axes, order)
    new_table, new_accum = pl.pallas_call(
        write_kernel,
        out_shape=(
            jax.ShapeDtypeStruct(table.shape, f32), jax.ShapeDtypeStruct(accum.shape, f32),
        ),
        in_specs=[vmem, vmem, vmem, hbm, hbm],
        out_specs=(hbm, hbm),
        scratch_shapes=[pltpu.SMEM((n // LANES, LANES), jnp.int32)] + held + [
            pltpu.SemaphoreType.DMA((COPIES,)), pltpu.SemaphoreType.DMA((COPIES,)),
            pltpu.SemaphoreType.DMA,
        ],
        cost_estimate=pl.CostEstimate(flops=10**9, transcendentals=0, bytes_accessed=8 * 2**20),
        compiler_params=pltpu.CompilerParams(vmem_limit_bytes=write_vmem),
        name="write",
    )(ids, new_t, new_a, *in_hbm(table, accum))
    fresh = pl.pallas_call(
        functools.partial(finish_kernel, cap, order),
        out_shape=jax.ShapeDtypeStruct((n, width), jnp.bfloat16),
        in_specs=[vmem],
        out_specs=vmem,
        compiler_params=pltpu.CompilerParams(vmem_limit_bytes=PACK_VMEM),
        name="finish",
    )(returned.reshape(-1, width))
    return (new_table, new_accum, fresh)


def solution(mesh):
    placed = (
        P(("aa", "ba"), None),
        P(("aa", "ba")),
        P(("aa", "ba")),
        P(("aa", "ba")),
        P(("aa", "ba"), None),
        P(("aa", "ba"), None),
    )
    return jax.shard_map(
        on_device,
        mesh=mesh,
        in_specs=placed,
        out_specs=(P(("aa", "ba"), None), P(("aa", "ba"), None), P(("aa", "ba"), None)),
        check_vma=False,
    )
```
